32 devices in a mesh: kpt: 2 (over x), gx: 16 (over z, y, core).
Axes of the slice: x: 2, y: 2, z: 4, core: 2. Of those that a mesh axis runs over, the one named last changes fastest.
Arguments:
- e_field: float32 [2, 3, 64, 512, 128], P(None, None, ('kpt', 'gx')), parts along dimension 2, may hold values from -6 to 6
- h_field: float32 [2, 3, 64, 512, 128], P(None, None, ('kpt', 'gx')), parts along dimension 2, may hold values from -6 to 6
- labels: int32 [64, 512, 128], P(('kpt', 'gx')), parts along dimension 0, may hold values from 0 to 3
- kpoint: int32 [4], P('kpt'), parts along dimension 0, may hold values from 0 to 15
- eps_inf: float32 [4], replicated, may hold values from 1 to 12
- delta_eps: float32 [4], replicated, may hold values from 0.5 to 4
- omega_zero: float32 [4], replicated, may hold values from 0.2 to 1
- damping: float32 [4], replicated, may hold values from 0.05 to 0.8
Outputs:
- e_final: float32 [2, 3, 64, 512, 128], P(None, None, ('kpt', 'gx')), parts along dimension 2
- h_final: float32 [2, 3, 64, 512, 128], P(None, None, ('kpt', 'gx')), parts along dimension 2
The draws below stay inside these ranges and needn't reach their ends.
There are 2 independent parts, one for each index of `kpt`. The reference program is written for one: setup_inputs(seed, part) draws one part's arguments, and reference() takes and returns one part's arrays. A program takes and returns all parts, laid end to end along the dimension named above; an argument that names none is the same for every part. Nothing has to cross between parts.
Inputs may be any that keep to these rules, and one draw needn't show every extreme that they name: `kpoint`: entry 0 indexes the k-point along x, entry 1 along y, out of 16 each.
All inputs are finite; a program needn't handle non-finite values.
Results may differ from the reference program's by a relative error of at most 0.00002.
Values sent between devices are 32-bit elements; how exact they have to be, the bound alone decides.
No kernel may reach another device: no remote copies, remote signals or barrier semaphores. Data moves between devices by JAX's collectives and lax.ppermute only.
A program may use at most 128 MiB of HBM per device.

```python
import math
import jax
import jax.numpy as jnp
from jax import lax

NY = 512
NZ = 128
ITERS = 12
LABELS = 4
KGRID = 16
NX = 32


def with_ends(entries, key, least, top_value):
    spot = [jax.random.randint(jax.random.fold_in(key, axis), (), 0, length) for axis, length in enumerate(entries.shape)]
    longest = entries.shape.index(max(entries.shape))
    beside = spot[:longest] + [(spot[longest] + 1) % entries.shape[longest]] + spot[longest + 1:]
    return entries.at[tuple(spot)].set(least).at[tuple(beside)].set(top_value)


def level_of(key, shape, split, smallest, largest):
    def one(dim, parts):
        draws = jax.random.uniform(jax.random.fold_in(jax.random.fold_in(key, 6), dim), (parts,), jnp.float32, smallest / len(split), largest / len(split))
        return jnp.repeat(jnp.exp(draws), shape[dim] // parts).reshape((-1,) + (1,) * (len(shape) - dim - 1))

    factor_of = one(*split[0])
    for cut in split[1:]:
        factor_of = factor_of * one(*cut)
    return factor_of


def noise(stream_key, shape, scale, bound, split=(), held_as=jnp.bfloat16):
    array = jax.random.normal(stream_key, shape, jnp.float32) * scale
    if len(split) > 0:
        array = level_of(stream_key, shape, split, -0.22, 0.18) * array
    return jnp.clip(array, min=-bound, max=bound).astype(held_as)


def setup_inputs(seed: int = 0, part: int = 0) -> dict:
    key_of = jax.random.split(jax.random.key(seed), 9)
    part_splits = jax.random.split(jax.random.fold_in(key_of[8], part), 9)
    return {
        "e_field": noise(part_splits[0], (2, 3, NX, NY, NZ), 1.0, 6.0, ((2, 16),), jnp.float32),
        "h_field": noise(part_splits[1], (2, 3, NX, NY, NZ), 1.0, 6.0, ((2, 16),), jnp.float32),
        "labels": with_ends(jax.random.randint(part_splits[2], (NX, NY, NZ), 0, LABELS), jax.random.fold_in(part_splits[2], 1), 0, LABELS - 1).astype(jnp.int32),
        "kpoint": jax.random.randint(part_splits[3], (2,), 0, KGRID).astype(jnp.int32),
        "eps_inf": jnp.clip(jnp.exp(jax.random.uniform(key_of[4], (LABELS,), jnp.float32, math.log(1.0), math.log(12.0))), 1.0, 12.0),
        "delta_eps": jnp.clip(jnp.exp(jax.random.uniform(key_of[5], (LABELS,), jnp.float32, math.log(0.5), math.log(4.0))), 0.5, 4.0),
        "omega_zero": jnp.clip(jnp.exp(jax.random.uniform(key_of[6], (LABELS,), jnp.float32, math.log(0.2), math.log(1.0))), 0.2, 1.0),
        "damping": jnp.clip(jnp.exp(jax.random.uniform(key_of[7], (LABELS,), jnp.float32, math.log(0.05), math.log(0.8))), 0.05, 0.8),
    }


time_step = 0.5


def cmul(field, cosv, sinv):
    return jnp.stack([field[0] * cosv - field[1] * sinv, field[0] * sinv + field[1] * cosv])


def next_axis(field, axis, cosv, sinv):
    rolled = jnp.roll(field, -1, axis=axis)
    count = field.shape[axis]
    inner = lax.slice_in_dim(rolled, 0, count - 1, axis=axis)
    last = cmul(lax.slice_in_dim(rolled, count - 1, count, axis=axis), cosv, sinv)
    return jnp.concatenate([inner, last], axis=axis)


def prev_axis(field, axis, cosv, sinv):
    rolled = jnp.roll(field, 1, axis=axis)
    count = field.shape[axis]
    first = cmul(lax.slice_in_dim(rolled, 0, 1, axis=axis), cosv, -sinv)
    inner = lax.slice_in_dim(rolled, 1, count, axis=axis)
    return jnp.concatenate([first, inner], axis=axis)


def next_z(field):
    zeros = jnp.zeros(field.shape[:-1] + (1,), jnp.float32)
    return jnp.concatenate([field[..., 1:], zeros], axis=-1)


def prev_z(field):
    zeros = jnp.zeros(field.shape[:-1] + (1,), jnp.float32)
    return jnp.concatenate([zeros, field[..., :-1]], axis=-1)


def per_cell(labels, table):
    picked = jnp.zeros(labels.shape, jnp.float32)
    for label in range(table.shape[0]):
        picked = picked + jnp.where(labels == label, table[label], jnp.float32(0.0))
    return picked


def reference(e_field, h_field, labels, kpoint, eps_inf, delta_eps, omega_zero, damping):
    theta_x = jnp.float32(2.0 * math.pi) * kpoint[0].astype(jnp.float32) / KGRID
    theta_y = jnp.float32(2.0 * math.pi) * kpoint[1].astype(jnp.float32) / KGRID
    cos_x, sin_x = jnp.cos(theta_x), jnp.sin(theta_x)
    cos_y, sin_y = jnp.cos(theta_y), jnp.sin(theta_y)
    half = damping * time_step / 2.0
    ce = per_cell(labels, time_step / eps_inf)
    ja = per_cell(labels, (1.0 - half) / (1.0 + half))
    jb = per_cell(labels, time_step * omega_zero * omega_zero / (1.0 + half))
    de = per_cell(labels, delta_eps)

    def advance(step, carry):
        efield, hfield, polar, current = carry
        ex, ey, ez = efield[:, 0], efield[:, 1], efield[:, 2]
        curl_x = (next_axis(ez, -2, cos_y, sin_y) - ez) - (next_z(ey) - ey)
        curl_y = (next_z(ex) - ex) - (next_axis(ez, -3, cos_x, sin_x) - ez)
        curl_z = (next_axis(ey, -3, cos_x, sin_x) - ey) - (next_axis(ex, -2, cos_y, sin_y) - ex)
        hfield = hfield - time_step * jnp.stack([curl_x, curl_y, curl_z], axis=1)
        hx, hy, hz = hfield[:, 0], hfield[:, 1], hfield[:, 2]
        kurl_x = (hz - prev_axis(hz, -2, cos_y, sin_y)) - (hy - prev_z(hy))
        kurl_y = (hx - prev_z(hx)) - (hz - prev_axis(hz, -3, cos_x, sin_x))
        kurl_z = (hy - prev_axis(hy, -3, cos_x, sin_x)) - (hx - prev_axis(hx, -2, cos_y, sin_y))
        kurl = jnp.stack([kurl_x, kurl_y, kurl_z], axis=1)
        current = ja * current + jb * (de * efield - polar)
        polar = polar + time_step * current
        efield = efield + ce * (kurl - current)
        return efield, hfield, polar, current

    zeros = jnp.zeros(e_field.shape, jnp.float32)
    efield, hfield, polar, current = lax.fori_loop(0, ITERS, advance, (e_field, h_field, zeros, zeros))
    return efield, hfield
```

```python
import functools
import math

import jax
import jax.numpy as jnp
from jax import lax
from jax.experimental import pallas as pl
from jax.experimental.pallas import tpu as pltpu
from jax.sharding import PartitionSpec as P

ITERS = 12
KGRID = 16
ROWS = 16
PARTS = 2
HEAD = 6
LIMIT = 6 * 1024 * 1024


time_step = 0.5


def shifted(value, axis, by):
    size = lax.axis_size(axis)
    return lax.ppermute(value, axis, [(i, (i + by) % size) for i in range(size)])


def lane_masks(shape):
    lane = lax.broadcasted_iota(jnp.int32, shape, 1)
    return lane == 0, lane == shape[1] - 1


def rotated(re, im, cosv, sinv):
    return re * cosv - im * sinv, re * sinv + im * cosv


def load_next_y(ref, comp, plane, row, wrap, cosv, sinv):
    if not wrap:
        return [ref[c, comp, plane, pl.ds(row + 1, ROWS), :] for c in range(2)]
    edge = rotated(ref[0, comp, plane, 0:1, :], ref[1, comp, plane, 0:1, :], cosv, sinv)
    found = []
    for c in range(2):
        rolled = pltpu.roll(ref[c, comp, plane, pl.ds(row, ROWS), :], ROWS - 1, 0)
        line = lax.broadcasted_iota(jnp.int32, rolled.shape, 0)
        found.append(jnp.where(line == ROWS - 1, edge[c], rolled))
    return found


def load_prev_y(ref, comp, plane, row, wrap, cosv, sinv):
    if not wrap:
        return [ref[c, comp, plane, pl.ds(row - 1, ROWS), :] for c in range(2)]
    ny = ref.shape[3]
    edge = rotated(ref[0, comp, plane, ny - 1 : ny, :], ref[1, comp, plane, ny - 1 : ny, :], cosv, -sinv)
    found = []
    for c in range(2):
        rolled = pltpu.roll(ref[c, comp, plane, pl.ds(row, ROWS), :], 1, 0)
        line = lax.broadcasted_iota(jnp.int32, rolled.shape, 0)
        found.append(jnp.where(line == 0, edge[c], rolled))
    return found


def over_rows(first, count, special, body):
    blocks = count // ROWS
    start, stop = 0, blocks
    if special == "first":
        body(first, first, True)
        start = 1
    if special == "last":
        stop = blocks - 1

    def one(step, _):
        row = pl.multiple_of(first + step * ROWS, ROWS)
        body(row, row - first, False)
        return 0

    lax.fori_loop(start, stop, one, 0, unroll=2)
    if special == "last":
        body(first + (blocks - 1) * ROWS, (blocks - 1) * ROWS, True)


def magnetic_kernel(first, count, special, phase, e, h, right, h_out, sent):
    planes = e.shape[2]
    lanes = e.shape[4]
    cx, sx, cy, sy = phase[0], phase[1], phase[2], phase[3]
    zero = jnp.zeros((ROWS, lanes), jnp.float32)
    _, last_lane = lane_masks((ROWS, lanes))

    def next_z(value):
        return jnp.where(last_lane, zero, pltpu.roll(value, lanes - 1, 1))

    def body(row, local, wrap):
        rows = pl.ds(row, ROWS)
        here = pl.ds(local, ROWS)
        for p in range(planes):
            if p + 1 < planes:
                ney = [e[c, 1, p + 1, rows, :] for c in range(2)]
                nez = [e[c, 2, p + 1, rows, :] for c in range(2)]
            else:
                ney = rotated(right[0, 0, here, :], right[1, 0, here, :], cx, sx)
                nez = rotated(right[0, 1, here, :], right[1, 1, here, :], cx, sx)
            yez = load_next_y(e, 2, p, row, wrap, cy, sy)
            yex = load_next_y(e, 0, p, row, wrap, cy, sy)
            for c in range(2):
                ex, ey, ez = (e[c, k, p, rows, :] for k in range(3))
                curl_x = (yez[c] - ez) - (next_z(ey) - ey)
                curl_y = (next_z(ex) - ex) - (nez[c] - ez)
                curl_z = (ney[c] - ey) - (yex[c] - ex)
                hx = h[c, 0, p, rows, :] - time_step * curl_x
                hy = h[c, 1, p, rows, :] - time_step * curl_y
                hz = h[c, 2, p, rows, :] - time_step * curl_z
                h_out[c, 0, p, rows, :] = hx
                h_out[c, 1, p, rows, :] = hy
                h_out[c, 2, p, rows, :] = hz
                if p == planes - 1:
                    sent[c, 0, here, :] = hy
                    sent[c, 1, here, :] = hz

    over_rows(first, count, special, body)


def electric_kernel(first, count, special, fresh, n_in, *refs):
    ins, outs = refs[:n_in], refs[n_in:]
    phase, h, left, ce_ref, ja_ref, jb_ref, de_ref, e = ins[:8]
    polar, current = (None, None) if fresh else ins[8:10]
    e_out, polar_out, current_out, sent = outs
    planes = e.shape[2]
    lanes = e.shape[4]
    cx, sx, cy, sy = phase[4], phase[5], phase[2], phase[3]
    zero = jnp.zeros((ROWS, lanes), jnp.float32)
    first_lane, _ = lane_masks((ROWS, lanes))

    def prev_z(value):
        return jnp.where(first_lane, zero, pltpu.roll(value, 1, 1))

    def body(row, local, wrap):
        rows = pl.ds(row, ROWS)
        here = pl.ds(local, ROWS)
        for p in range(planes):
            if p > 0:
                phy = [h[c, 1, p - 1, rows, :] for c in range(2)]
                phz = [h[c, 2, p - 1, rows, :] for c in range(2)]
            else:
                phy = rotated(left[0, 0, here, :], left[1, 0, here, :], cx, sx)
                phz = rotated(left[0, 1, here, :], left[1, 1, here, :], cx, sx)
            yhz = load_prev_y(h, 2, p, row, wrap, cy, sy)
            yhx = load_prev_y(h, 0, p, row, wrap, cy, sy)
            ce, ja, jb, de = (t[p, rows, :] for t in (ce_ref, ja_ref, jb_ref, de_ref))
            for c in range(2):
                hx, hy, hz = (h[c, k, p, rows, :] for k in range(3))
                kurls = (
                    (hz - yhz[c]) - (hy - prev_z(hy)),
                    (hx - prev_z(hx)) - (hz - phz[c]),
                    (hy - phy[c]) - (hx - yhx[c]),
                )
                for k in range(3):
                    field = e[c, k, p, rows, :]
                    if fresh:
                        cur = jb * (de * field)
                        pol = time_step * cur
                    else:
                        pol = polar[c, k, p, rows, :]
                        cur = ja * current[c, k, p, rows, :] + jb * (de * field - pol)
                        pol = pol + time_step * cur
                    field = field + ce * (kurls[k] - cur)
                    e_out[c, k, p, rows, :] = field
                    polar_out[c, k, p, rows, :] = pol
                    current_out[c, k, p, rows, :] = cur
                    if p == 0 and k > 0:
                        sent[c, k - 1, here, :] = field

    over_rows(first, count, special, body)


def load_kernel(scalars, e_in, h_in, labels, e, h, ce, ja, jb, de, held, sems):
    copies = [
        pltpu.make_async_copy(labels, held, sems.at[0]),
        pltpu.make_async_copy(e_in, e, sems.at[1]),
        pltpu.make_async_copy(h_in, h, sems.at[2]),
    ]
    for copy in copies:
        copy.start()
    copies[0].wait()
    count = (scalars.shape[0] - HEAD) // 4

    def one(step, _):
        rows = pl.ds(pl.multiple_of(step * ROWS, ROWS), ROWS)
        for p in range(held.shape[0]):
            label = held[p, rows, :]
            for t, table in enumerate((ce, ja, jb, de)):
                picked = jnp.zeros(label.shape, jnp.float32)
                for k in range(count):
                    picked = jnp.where(label == k, scalars[HEAD + t * count + k], picked)
                table[p, rows, :] = picked
        return 0

    lax.fori_loop(0, held.shape[1] // ROWS, one, 0)
    copies[1].wait()
    copies[2].wait()


VM = pl.BlockSpec(memory_space=pltpu.VMEM)
SM = pl.BlockSpec(memory_space=pltpu.SMEM)


def load(scalars, e_field, h_field, labels):
    field = pltpu.VMEM(e_field.shape, jnp.float32)
    table = pltpu.VMEM(labels.shape, jnp.float32)
    hbm = pl.BlockSpec(memory_space=pltpu.HBM)
    return pl.pallas_call(
        load_kernel,
        out_shape=(field, field, table, table, table, table),
        in_specs=[SM, hbm, hbm, hbm],
        out_specs=(VM,) * 6,
        scratch_shapes=[pltpu.VMEM(labels.shape, jnp.int32), pltpu.SemaphoreType.DMA((3,))],
        cost_estimate=pl.CostEstimate(flops=8 * e_field.size, bytes_accessed=8 * e_field.size, transcendentals=0),
        compiler_params=pltpu.CompilerParams(vmem_limit_bytes=LIMIT),
        name="load",
    )(scalars, e_field, h_field, labels)


def advance_magnetic(part, phase, e, h, right):
    ny = e.shape[3]
    count = ny // PARTS
    special = "last" if part == PARTS - 1 else None
    n_vec = math.prod(e.shape) // PARTS
    return pl.pallas_call(
        functools.partial(magnetic_kernel, part * count, count, special),
        out_shape=(
            pltpu.VMEM(h.shape, jnp.float32),
            pltpu.VMEM(right.shape, jnp.float32),
        ),
        in_specs=[SM, VM, VM, VM],
        out_specs=(VM, VM),
        input_output_aliases={2: 0},
        cost_estimate=pl.CostEstimate(flops=6 * n_vec, bytes_accessed=12 * n_vec, transcendentals=0),
        compiler_params=pltpu.CompilerParams(vmem_limit_bytes=LIMIT),
        name="magnetic",
    )(phase, e, h, right)


def advance_electric(part, fresh, phase, h, left, coeffs, e, polar, current):
    ny = e.shape[3]
    count = ny // PARTS
    special = "first" if part == 0 else None
    n_vec = math.prod(e.shape) // PARTS
    operands = [phase, h, left, *coeffs, e]
    aliases = {7: 0}
    if polar is not None:
        operands += [polar, current]
        aliases.update({8: 1, 9: 2})
    shape = pltpu.VMEM(e.shape, jnp.float32)
    return pl.pallas_call(
        functools.partial(electric_kernel, part * count, count, special, fresh, len(operands)),
        out_shape=(shape, shape, shape, pltpu.VMEM(left.shape, jnp.float32)),
        in_specs=[SM] + [VM] * (len(operands) - 1),
        out_specs=(VM,) * 4,
        input_output_aliases=aliases,
        cost_estimate=pl.CostEstimate(flops=14 * n_vec, bytes_accessed=32 * n_vec, transcendentals=0),
        compiler_params=pltpu.CompilerParams(vmem_limit_bytes=LIMIT),
        name="electric",
    )(*operands)


def shards(e_field, h_field, labels, kpoint, eps_inf, delta_eps, omega_zero, damping):
    theta_x = jnp.float32(2.0 * math.pi) * kpoint[0].astype(jnp.float32) / KGRID
    theta_y = jnp.float32(2.0 * math.pi) * kpoint[1].astype(jnp.float32) / KGRID
    cos_x, sin_x = (jnp.cos(theta_x), jnp.sin(theta_x))
    cos_y, sin_y = (jnp.cos(theta_y), jnp.sin(theta_y))
    half = damping * time_step / 2.0
    tables = (
        time_step / eps_inf,
        (1.0 - half) / (1.0 + half),
        time_step * omega_zero * omega_zero / (1.0 + half),
        delta_eps,
    )
    position = lax.axis_index("gx")
    at_first = position == 0
    at_last = position == lax.axis_size("gx") - 1
    one, none = jnp.float32(1.0), jnp.float32(0.0)
    phase = jnp.stack(
        [
            jnp.where(at_last, cos_x, one),
            jnp.where(at_last, sin_x, none),
            cos_y,
            sin_y,
            jnp.where(at_first, cos_x, one),
            jnp.where(at_first, -sin_x, none),
        ]
    )
    phase = jnp.concatenate([phase, *tables])
    efield, hfield, *coeffs = load(phase, e_field, h_field, labels)
    polar = current = None
    count = e_field.shape[3] // PARTS
    right = [
        shifted(e_field[:, 1:3, 0, q * count : (q + 1) * count], "gx", -1) for q in range(PARTS)
    ]
    for step in range(ITERS):
        left = []
        for q in range(PARTS):
            hfield, sent = advance_magnetic(q, phase, efield, hfield, right[q])
            left.append(shifted(sent, "gx", 1))
        right = []
        for q in range(PARTS):
            efield, polar, current, sent = advance_electric(
                q, step == 0, phase, hfield, left[q], coeffs, efield, polar, current
            )
            if step + 1 < ITERS:
                right.append(shifted(sent, "gx", -1))
    return (efield, hfield)


def solution(mesh):
    placed = (
        P(None, None, ("kpt", "gx"), None, None),
        P(None, None, ("kpt", "gx"), None, None),
        P(("kpt", "gx"), None, None),
        P("kpt"),
        P(),
        P(),
        P(),
        P(),
    )
    return jax.shard_map(
        shards,
        mesh=mesh,
        in_specs=placed,
        out_specs=(
            P(None, None, ("kpt", "gx"), None, None),
            P(None, None, ("kpt", "gx"), None, None),
        ),
        check_vma=False,
    )
```

```python
import functools
import math

import jax
import jax.numpy as jnp
from jax import lax
from jax.experimental import pallas as pl
from jax.experimental.pallas import tpu as pltpu
from jax.sharding import PartitionSpec as P

ITERS = 12
KGRID = 16
ROWS = 16
PARTS = 4
HEAD = 6
LIMIT = 6 * 1024 * 1024


time_step = 0.5


def shifted(value, axis, by):
    size = lax.axis_size(axis)
    return lax.ppermute(value, axis, [(i, (i + by) % size) for i in range(size)])


def lane_masks(shape):
    lane = lax.broadcasted_iota(jnp.int32, shape, 1)
    return lane == 0, lane == shape[1] - 1


def rotated(re, im, cosv, sinv):
    return re * cosv - im * sinv, re * sinv + im * cosv


def load_next_y(ref, comp, plane, row, wrap, cosv, sinv):
    if not wrap:
        return [ref[c, comp, plane, pl.ds(row + 1, ROWS), :] for c in range(2)]
    edge = rotated(ref[0, comp, plane, 0:1, :], ref[1, comp, plane, 0:1, :], cosv, sinv)
    found = []
    for c in range(2):
        rolled = pltpu.roll(ref[c, comp, plane, pl.ds(row, ROWS), :], ROWS - 1, 0)
        line = lax.broadcasted_iota(jnp.int32, rolled.shape, 0)
        found.append(jnp.where(line == ROWS - 1, edge[c], rolled))
    return found


def load_prev_y(ref, comp, plane, row, wrap, cosv, sinv):
    if not wrap:
        return [ref[c, comp, plane, pl.ds(row - 1, ROWS), :] for c in range(2)]
    ny = ref.shape[3]
    edge = rotated(ref[0, comp, plane, ny - 1 : ny, :], ref[1, comp, plane, ny - 1 : ny, :], cosv, -sinv)
    found = []
    for c in range(2):
        rolled = pltpu.roll(ref[c, comp, plane, pl.ds(row, ROWS), :], 1, 0)
        line = lax.broadcasted_iota(jnp.int32, rolled.shape, 0)
        found.append(jnp.where(line == 0, edge[c], rolled))
    return found


def over_rows(first, count, special, body):
    blocks = count // ROWS
    start, stop = 0, blocks
    if special == "first":
        body(first, first, True)
        start = 1
    if special == "last":
        stop = blocks - 1

    def one(step, _):
        row = pl.multiple_of(first + step * ROWS, ROWS)
        body(row, row - first, False)
        return 0

    lax.fori_loop(start, stop, one, 0, unroll=2)
    if special == "last":
        body(first + (blocks - 1) * ROWS, (blocks - 1) * ROWS, True)


def magnetic_kernel(first, count, special, own, phase, e, h, *refs):
    right, h_out, sent = refs if len(refs) == 3 else (None, refs[0], None)
    planes = e.shape[2]
    lanes = e.shape[4]
    cx, sx, cy, sy = phase[0], phase[1], phase[2], phase[3]
    zero = jnp.zeros((ROWS, lanes), jnp.float32)
    _, last_lane = lane_masks((ROWS, lanes))

    def next_z(value):
        return jnp.where(last_lane, zero, pltpu.roll(value, lanes - 1, 1))

    def body(row, local, wrap):
        rows = pl.ds(row, ROWS)
        here = pl.ds(local, ROWS)
        for p in own:
            if p + 1 < planes:
                ney = [e[c, 1, p + 1, rows, :] for c in range(2)]
                nez = [e[c, 2, p + 1, rows, :] for c in range(2)]
            else:
                ney = rotated(right[0, 0, here, :], right[1, 0, here, :], cx, sx)
                nez = rotated(right[0, 1, here, :], right[1, 1, here, :], cx, sx)
            yez = load_next_y(e, 2, p, row, wrap, cy, sy)
            yex = load_next_y(e, 0, p, row, wrap, cy, sy)
            for c in range(2):
                ex, ey, ez = (e[c, k, p, rows, :] for k in range(3))
                curl_x = (yez[c] - ez) - (next_z(ey) - ey)
                curl_y = (next_z(ex) - ex) - (nez[c] - ez)
                curl_z = (ney[c] - ey) - (yex[c] - ex)
                hx = h[c, 0, p, rows, :] - time_step * curl_x
                hy = h[c, 1, p, rows, :] - time_step * curl_y
                hz = h[c, 2, p, rows, :] - time_step * curl_z
                h_out[c, 0, p, rows, :] = hx
                h_out[c, 1, p, rows, :] = hy
                h_out[c, 2, p, rows, :] = hz
                if sent is not None:
                    sent[c, 0, here, :] = hy
                    sent[c, 1, here, :] = hz

    over_rows(first, count, special, body)


def electric_kernel(first, count, special, fresh, own, n_in, *refs):
    ins, outs = list(refs[:n_in]), refs[n_in:]
    left = ins.pop() if own[0] == 0 else None
    phase, h, ce_ref, ja_ref, jb_ref, de_ref, e = ins[:7]
    polar, current = (None, None) if fresh else ins[7:9]
    e_out, polar_out, current_out = outs[:3]
    sent = outs[3] if len(outs) > 3 else None
    planes = e.shape[2]
    lanes = e.shape[4]
    cx, sx, cy, sy = phase[4], phase[5], phase[2], phase[3]
    zero = jnp.zeros((ROWS, lanes), jnp.float32)
    first_lane, _ = lane_masks((ROWS, lanes))

    def prev_z(value):
        return jnp.where(first_lane, zero, pltpu.roll(value, 1, 1))

    def body(row, local, wrap):
        rows = pl.ds(row, ROWS)
        here = pl.ds(local, ROWS)
        for p in own:
            if p > 0:
                phy = [h[c, 1, p - 1, rows, :] for c in range(2)]
                phz = [h[c, 2, p - 1, rows, :] for c in range(2)]
            else:
                phy = rotated(left[0, 0, here, :], left[1, 0, here, :], cx, sx)
                phz = rotated(left[0, 1, here, :], left[1, 1, here, :], cx, sx)
            yhz = load_prev_y(h, 2, p, row, wrap, cy, sy)
            yhx = load_prev_y(h, 0, p, row, wrap, cy, sy)
            ce, ja, jb, de = (t[p, rows, :] for t in (ce_ref, ja_ref, jb_ref, de_ref))
            for c in range(2):
                hx, hy, hz = (h[c, k, p, rows, :] for k in range(3))
                kurls = (
                    (hz - yhz[c]) - (hy - prev_z(hy)),
                    (hx - prev_z(hx)) - (hz - phz[c]),
                    (hy - phy[c]) - (hx - yhx[c]),
                )
                for k in range(3):
                    field = e[c, k, p, rows, :]
                    if fresh:
                        cur = jb * (de * field)
                        pol = time_step * cur
                    else:
                        pol = polar[c, k, p, rows, :]
                        cur = ja * current[c, k, p, rows, :] + jb * (de * field - pol)
                        pol = pol + time_step * cur
                    field = field + ce * (kurls[k] - cur)
                    e_out[c, k, p, rows, :] = field
                    polar_out[c, k, p, rows, :] = pol
                    current_out[c, k, p, rows, :] = cur
                    if sent is not None and k > 0:
                        sent[c, k - 1, here, :] = field

    over_rows(first, count, special, body)


def load_kernel(scalars, e_in, h_in, labels, e, h, ce, ja, jb, de, held, sems):
    copies = [
        pltpu.make_async_copy(labels, held, sems.at[0]),
        pltpu.make_async_copy(e_in, e, sems.at[1]),
        pltpu.make_async_copy(h_in, h, sems.at[2]),
    ]
    for copy in copies:
        copy.start()
    copies[0].wait()
    count = (scalars.shape[0] - HEAD) // 4

    def one(step, _):
        rows = pl.ds(pl.multiple_of(step * ROWS, ROWS), ROWS)
        for p in range(held.shape[0]):
            label = held[p, rows, :]
            for t, table in enumerate((ce, ja, jb, de)):
                picked = jnp.zeros(label.shape, jnp.float32)
                for k in range(count):
                    picked = jnp.where(label == k, scalars[HEAD + t * count + k], picked)
                table[p, rows, :] = picked
        return 0

    lax.fori_loop(0, held.shape[1] // ROWS, one, 0)
    copies[1].wait()
    copies[2].wait()


VM = pl.BlockSpec(memory_space=pltpu.VMEM)
SM = pl.BlockSpec(memory_space=pltpu.SMEM)


def load(scalars, e_field, h_field, labels):
    field = pltpu.VMEM(e_field.shape, jnp.float32)
    table = pltpu.VMEM(labels.shape, jnp.float32)
    hbm = pl.BlockSpec(memory_space=pltpu.HBM)
    return pl.pallas_call(
        load_kernel,
        out_shape=(field, field, table, table, table, table),
        in_specs=[SM, hbm, hbm, hbm],
        out_specs=(VM,) * 6,
        scratch_shapes=[pltpu.VMEM(labels.shape, jnp.int32), pltpu.SemaphoreType.DMA((3,))],
        cost_estimate=pl.CostEstimate(flops=8 * e_field.size, bytes_accessed=8 * e_field.size, transcendentals=0),
        compiler_params=pltpu.CompilerParams(vmem_limit_bytes=LIMIT),
        name="load",
    )(scalars, e_field, h_field, labels)


def advance_magnetic(part, own, phase, e, h, right):
    ny, planes = e.shape[3], e.shape[2]
    count = ny // PARTS
    special = "last" if part == PARTS - 1 else None
    n_vec = math.prod(e.shape) // PARTS * len(own) // planes
    operands, out_shape = [phase, e, h], [pltpu.VMEM(h.shape, jnp.float32)]
    if right is not None:
        operands.append(right)
        out_shape.append(pltpu.VMEM(right.shape, jnp.float32))
    return pl.pallas_call(
        functools.partial(magnetic_kernel, part * count, count, special, own),
        out_shape=tuple(out_shape),
        in_specs=[SM] + [VM] * (len(operands) - 1),
        out_specs=(VM,) * len(out_shape),
        input_output_aliases={2: 0},
        cost_estimate=pl.CostEstimate(flops=6 * n_vec, bytes_accessed=12 * n_vec, transcendentals=0),
        compiler_params=pltpu.CompilerParams(vmem_limit_bytes=LIMIT),
        name="magnetic",
    )(*operands)


def advance_electric(part, own, fresh, phase, h, left, coeffs, e, polar, current, send):
    ny, planes = e.shape[3], e.shape[2]
    count = ny // PARTS
    special = "first" if part == 0 else None
    n_vec = math.prod(e.shape) // PARTS * len(own) // planes
    operands = [phase, h, *coeffs, e]
    aliases = {6: 0}
    if polar is not None:
        operands += [polar, current]
        aliases.update({7: 1, 8: 2})
    out_shape = [pltpu.VMEM(e.shape, jnp.float32)] * 3
    if left is not None:
        operands.append(left)
        if send:
            out_shape.append(pltpu.VMEM(left.shape, jnp.float32))
    return pl.pallas_call(
        functools.partial(electric_kernel, part * count, count, special, fresh, own, len(operands)),
        out_shape=tuple(out_shape),
        in_specs=[SM] + [VM] * (len(operands) - 1),
        out_specs=(VM,) * len(out_shape),
        input_output_aliases=aliases,
        cost_estimate=pl.CostEstimate(flops=14 * n_vec, bytes_accessed=32 * n_vec, transcendentals=0),
        compiler_params=pltpu.CompilerParams(vmem_limit_bytes=LIMIT),
        name="electric",
    )(*operands)


def shards(e_field, h_field, labels, kpoint, eps_inf, delta_eps, omega_zero, damping):
    theta_x = jnp.float32(2.0 * math.pi) * kpoint[0].astype(jnp.float32) / KGRID
    theta_y = jnp.float32(2.0 * math.pi) * kpoint[1].astype(jnp.float32) / KGRID
    cos_x, sin_x = (jnp.cos(theta_x), jnp.sin(theta_x))
    cos_y, sin_y = (jnp.cos(theta_y), jnp.sin(theta_y))
    half = damping * time_step / 2.0
    tables = (
        time_step / eps_inf,
        (1.0 - half) / (1.0 + half),
        time_step * omega_zero * omega_zero / (1.0 + half),
        delta_eps,
    )
    position = lax.axis_index("gx")
    at_first = position == 0
    at_last = position == lax.axis_size("gx") - 1
    one, none = jnp.float32(1.0), jnp.float32(0.0)
    phase = jnp.stack(
        [
            jnp.where(at_last, cos_x, one),
            jnp.where(at_last, sin_x, none),
            cos_y,
            sin_y,
            jnp.where(at_first, cos_x, one),
            jnp.where(at_first, -sin_x, none),
        ]
    )
    phase = jnp.concatenate([phase, *tables])
    efield, hfield, *coeffs = load(phase, e_field, h_field, labels)
    polar = current = None
    count = e_field.shape[3] // PARTS
    right = [
        shifted(e_field[:, 1:3, 0, q * count : (q + 1) * count], "gx", -1) for q in range(PARTS)
    ]
    planes = e_field.shape[2]
    for step in range(ITERS):
        left = []
        for q in range(PARTS):
            hfield, sent = advance_magnetic(q, (planes - 1,), phase, efield, hfield, right[q])
            left.append(shifted(sent, "gx", 1))
            if planes > 1:
                own = tuple(range(planes - 1))
                (hfield,) = advance_magnetic(q, own, phase, efield, hfield, None)
        right = []
        for q in range(PARTS):
            more = step + 1 < ITERS
            efield, polar, current, *sent = advance_electric(
                q, (0,), step == 0, phase, hfield, left[q], coeffs, efield, polar, current, more
            )
            if more:
                right.append(shifted(sent[0], "gx", -1))
            if planes > 1:
                own = tuple(range(1, planes))
                efield, polar, current = advance_electric(
                    q, own, step == 0, phase, hfield, None, coeffs, efield, polar, current, False
                )
    return (efield, hfield)


def solution(mesh):
    placed = (
        P(None, None, ("kpt", "gx"), None, None),
        P(None, None, ("kpt", "gx"), None, None),
        P(("kpt", "gx"), None, None),
        P("kpt"),
        P(),
        P(),
        P(),
        P(),
    )
    return jax.shard_map(
        shards,
        mesh=mesh,
        in_specs=placed,
        out_specs=(
            P(None, None, ("kpt", "gx"), None, None),
            P(None, None, ("kpt", "gx"), None, None),
        ),
        check_vma=False,
    )
```
